8 devices in a mesh: dz: 2 (over z, y), dy: 2 (over x), dx: 2 (over core).
Axes of the slice: x: 2, y: 2, z: 1, core: 2. Of those that a mesh axis runs over, the one named last changes fastest.
Arguments:
- x_one: bfloat16 [16384, 2048], P(('dz', 'dy', 'dx'))
- g_one: bfloat16 [16384, 2048], P(('dz', 'dy', 'dx'))
- x_two: bfloat16 [16384, 2048], P(('dz', 'dy', 'dx'))
- g_two: bfloat16 [16384, 2048], P(('dz', 'dy', 'dx'))
- w_one: bfloat16 [2048, 5120], replicated
- w_two: bfloat16 [5120, 2048], replicated
- w_three: bfloat16 [2048, 5120], replicated
- w_four: bfloat16 [5120, 2048], replicated
Outputs:
- output 1: float32 [2048, 5120], replicated
- output 2: float32 [5120, 2048], replicated
- output 3: float32 [2048, 5120], replicated
- output 4: float32 [5120, 2048], replicated
- output 5: bfloat16 [16384, 2048], P(('dz', 'dy', 'dx'))
- output 6: bfloat16 [16384, 2048], P(('dz', 'dy', 'dx'))
All inputs are finite; a program needn't handle non-finite values.
Results may differ from the reference program's by a relative error of at most 0.00494.
Values are sent between devices in bfloat16 or wider.
A program may use at most 1.25 GiB of HBM per device.

```python
import jax
import jax.numpy as jnp
from jax import lax

D = 2048
FF = 5120
TOKENS_DEV = 2048
DEVICES = 8

GELU_C = 0.7978845608028654
GELU_A = 0.044715


def gelu_value(pre_act):
    pre_f = pre_act.astype(jnp.float32)
    return 0.5 * pre_f * (1.0 + jnp.tanh(GELU_C * (pre_f + GELU_A * pre_f * pre_f * pre_f)))


def gelu_slope(pre_act):
    pre_f = pre_act.astype(jnp.float32)
    tanh_val = jnp.tanh(GELU_C * (pre_f + GELU_A * pre_f * pre_f * pre_f))
    return 0.5 * (1.0 + tanh_val) + 0.5 * pre_f * (1.0 - tanh_val * tanh_val) * GELU_C * (1.0 + 3.0 * GELU_A * pre_f * pre_f)


def local_grads(x_rows, g_rows, w_one, w_two, w_three, w_four):
    pre_one = jnp.dot(x_rows, w_one, preferred_element_type=jnp.float32).astype(jnp.bfloat16)
    act_one = gelu_value(pre_one).astype(jnp.bfloat16)
    act_two = (jnp.dot(act_one, w_two, preferred_element_type=jnp.float32) + x_rows.astype(jnp.float32)).astype(jnp.bfloat16)
    pre_three = jnp.dot(act_two, w_three, preferred_element_type=jnp.float32).astype(jnp.bfloat16)
    act_three = gelu_value(pre_three).astype(jnp.bfloat16)
    grad_four = jnp.dot(act_three.T, g_rows, preferred_element_type=jnp.float32)
    dz_three = (jnp.dot(g_rows, w_four.T, preferred_element_type=jnp.float32) * gelu_slope(pre_three)).astype(jnp.bfloat16)
    grad_three = jnp.dot(act_two.T, dz_three, preferred_element_type=jnp.float32)
    dh_two = (jnp.dot(dz_three, w_three.T, preferred_element_type=jnp.float32) + g_rows.astype(jnp.float32)).astype(jnp.bfloat16)
    grad_two = jnp.dot(act_one.T, dh_two, preferred_element_type=jnp.float32)
    dz_one = (jnp.dot(dh_two, w_two.T, preferred_element_type=jnp.float32) * gelu_slope(pre_one)).astype(jnp.bfloat16)
    grad_one = jnp.dot(x_rows.T, dz_one, preferred_element_type=jnp.float32)
    dx_rows = (jnp.dot(dz_one, w_one.T, preferred_element_type=jnp.float32) + dh_two.astype(jnp.float32)).astype(jnp.bfloat16)
    return (grad_one, grad_two, grad_three, grad_four), dx_rows


def setup_inputs(seed: int = 0) -> dict:
    sub_keys = jax.random.split(jax.random.key(seed), 8)
    total_rows = DEVICES * TOKENS_DEV

    def normal_bf16(sub_key, shape, scale):
        return (jax.random.normal(sub_key, shape, jnp.float32) * scale).astype(jnp.bfloat16)

    return {
        "x_one": normal_bf16(sub_keys[0], (total_rows, D), 1.0),
        "g_one": normal_bf16(sub_keys[1], (total_rows, D), 1.0),
        "x_two": normal_bf16(sub_keys[2], (total_rows, D), 1.0),
        "g_two": normal_bf16(sub_keys[3], (total_rows, D), 1.0),
        "w_one": normal_bf16(sub_keys[4], (D, FF), D ** -0.5),
        "w_two": normal_bf16(sub_keys[5], (FF, D), FF ** -0.5),
        "w_three": normal_bf16(sub_keys[6], (D, FF), D ** -0.5),
        "w_four": normal_bf16(sub_keys[7], (FF, D), FF ** -0.5),
    }


def reference(x_one, g_one, x_two, g_two, w_one, w_two, w_three, w_four):
    block_shape = (DEVICES, TOKENS_DEV, D)
    blocks_in = (x_one.reshape(block_shape), g_one.reshape(block_shape), x_two.reshape(block_shape), g_two.reshape(block_shape))

    def device_step(acc_grads, block_in):
        x_first, g_first, x_second, g_second = block_in
        grads_first, dx_first = local_grads(x_first, g_first, w_one, w_two, w_three, w_four)
        grads_second, dx_second = local_grads(x_second, g_second, w_one, w_two, w_three, w_four)
        new_acc = tuple(acc_part + grad_a + grad_b for acc_part, grad_a, grad_b in zip(acc_grads, grads_first, grads_second))
        return new_acc, (dx_first, dx_second)

    zero_grads = (jnp.zeros((D, FF), jnp.float32), jnp.zeros((FF, D), jnp.float32), jnp.zeros((D, FF), jnp.float32), jnp.zeros((FF, D), jnp.float32))
    sum_grads, dx_blocks = lax.scan(device_step, zero_grads, blocks_in)
    mean_grads = [total_grad / DEVICES for total_grad in sum_grads]
    dx_first_all = dx_blocks[0].reshape(DEVICES * TOKENS_DEV, D)
    dx_second_all = dx_blocks[1].reshape(DEVICES * TOKENS_DEV, D)
    return (mean_grads[0], mean_grads[1], mean_grads[2], mean_grads[3], dx_first_all, dx_second_all)
```

```python
import jax
import jax.numpy as jnp
from jax import lax
from jax.experimental import pallas as pl
from jax.experimental.pallas import tpu as pltpu
from jax.sharding import PartitionSpec as P

GELU_C = 0.7978845608028654
GELU_A = 0.044715
SWAP = [(0, 1), (1, 0)]
FF_TILE = 512


STEPS = (
    ("F1", 0), ("F1", 1), ("F2", 0), ("F2", 1),
    ("F3", 0, 0), ("F3", 0, 1), ("S", 4, 0), ("F3", 1, 0), ("C", 4, 0), ("F3", 1, 1), ("S", 4, 1), ("K", 4, 0), ("C", 4, 1), ("K", 4, 1),
    ("U", 4, 0), ("B3", 0, 0), ("B3", 0, 1), ("S", 3, 0), ("G", 4, 0), ("U", 4, 1), ("B3", 1, 0), ("C", 3, 0), ("B3", 1, 1), ("S", 3, 1), ("G", 4, 1),
    ("K", 3, 0), ("C", 3, 1), ("K", 3, 1), ("B2", 0), ("U", 3, 0), ("B2", 1), ("S", 2, 0), ("S", 2, 1), ("U", 3, 1), ("C", 2, 0), ("B1", 0, 0),
    ("C", 2, 1), ("B1", 0, 1), ("G", 3, 0), ("S", 1, 0), ("B1", 1, 0), ("C", 1, 0), ("B1", 1, 1), ("G", 3, 1), ("S", 1, 1), ("K", 2, 0), ("C", 1, 1), ("U", 2, 0),
    ("K", 2, 1), ("K", 1, 0), ("U", 2, 1), ("K", 1, 1), ("BX", 0), ("G", 2, 0), ("BX", 1), ("R", 4), ("G", 2, 1), ("U", 1, 0), ("R", 3),
    ("U", 1, 1), ("G", 1, 0), ("G", 1, 1), ("R", 2), ("R", 1),
)


def gelu_value(pre_act):
    pre_f = pre_act.astype(jnp.float32)
    return 0.5 * pre_f * (1.0 + jnp.tanh(GELU_C * (pre_f + GELU_A * pre_f * pre_f * pre_f)))


def gelu_slope(pre_act):
    pre_f = pre_act.astype(jnp.float32)
    square = pre_f * pre_f
    tanh_val = jnp.tanh(pre_f * (GELU_C + (GELU_C * GELU_A) * square))
    return (0.5 + 0.5 * tanh_val) * (1.0 + (pre_f * (1.0 - tanh_val)) * (GELU_C + (3.0 * GELU_C * GELU_A) * square))


def mat_nn(left_op, right_op):
    return jnp.dot(left_op, right_op, preferred_element_type=jnp.float32)


def mat_nt(left_op, right_op):
    return lax.dot_general(left_op, right_op, (((1,), (1,)), ((), ())), preferred_element_type=jnp.float32)


def mat_tn(left_op, right_op):
    return lax.dot_general(left_op, right_op, (((0,), (0,)), ((), ())), preferred_element_type=jnp.float32)


def grad_blocks(dim_ops, ff_ops, blocks, offset, wide_first, block):
    count = len(dim_ops)
    rows = dim_ops[0].shape[0]
    half = 10 * block
    tiles = half // FF_TILE

    def body(blocks_ref, *refs):
        dim_refs, ff_refs, out_refs = refs[: 4 * count], refs[4 * count : 5 * count], refs[5 * count :]
        for i in range(4):
            value = None
            for m in range(count):
                dim_val, ff_val = dim_refs[4 * m + i][...], ff_refs[m][...]
                term = mat_tn(ff_val, dim_val) if wide_first else mat_tn(dim_val, ff_val)
                value = term if value is None else value + term
            lo = (i % 2) * block
            if wide_first:
                out_refs[i // 2][:, lo : lo + block] = value
            else:
                out_refs[i // 2][lo : lo + block, :] = value

    def dim_spec(i):
        return pl.BlockSpec((rows, block), lambda j, b: (0, b[i]))

    if wide_first:
        out_shape = jax.ShapeDtypeStruct((half, 2 * block), jnp.float32)
        out_spec = pl.BlockSpec((FF_TILE, 2 * block), lambda j, b: (j, 0))
    else:
        out_shape = jax.ShapeDtypeStruct((2 * block, half), jnp.float32)
        out_spec = pl.BlockSpec((2 * block, FF_TILE), lambda j, b: (0, j))
    return pl.pallas_call(
        body,
        grid_spec=pltpu.PrefetchScalarGridSpec(
            num_scalar_prefetch=1,
            grid=(tiles,),
            in_specs=[dim_spec(i) for _ in range(count) for i in range(4)]
            + [pl.BlockSpec((rows, FF_TILE), lambda j, b: (0, offset * tiles + j)) for _ in range(count)],
            out_specs=[out_spec, out_spec],
        ),
        out_shape=[out_shape, out_shape],
        compiler_params=pltpu.CompilerParams(vmem_limit_bytes=62 * 1024 * 1024, dimension_semantics=("arbitrary",)),
        cost_estimate=pl.CostEstimate(flops=8 * count * rows * block * half, bytes_accessed=2 * count * rows * (half + 4 * block) + 16 * block * half, transcendentals=0),
    )(blocks, *[op for op in dim_ops for _ in range(4)], *ff_ops)


def solution(mesh):
    dev_count = mesh.shape["dz"] * mesh.shape["dy"] * mesh.shape["dx"]
    row_spec = P(("dz", "dy", "dx"), None)
    rep_spec = P(None, None)

    def per_device(x_one, g_one, x_two, g_two, w_one, w_two, w_three, w_four):
        dim, ff = w_one.shape
        block = dim // dev_count
        half_ff = ff // 2
        idx_z, idx_y, idx_c = lax.axis_index("dz"), lax.axis_index("dy"), lax.axis_index("dx")
        anchor = [x_one]

        def at(*vals):
            out = lax.optimization_barrier((*vals, anchor[0]))[:-1]
            return out if len(out) > 1 else out[0]

        def mark(val):
            anchor[0] = val
            return val

        def block_ids(color, send):
            ids = []
            for core in (1 - idx_c, idx_c):
                if color == 0:
                    col = 1 - idx_y if send else idx_y
                    ids += [4 * core + 2 * (1 - idx_z) + col, 4 * core + 2 * idx_z + col]
                else:
                    row = 1 - idx_z if send else idx_z
                    ids += [4 * core + 2 * row + 1 - idx_y, 4 * core + 2 * row + idx_y]
            return jnp.stack(ids).astype(jnp.int32)

        ids = {(color, send): block_ids(color, send) for color in (0, 1) for send in (False, True)}

        class Grad:
            def __init__(self, dim_ops, wide_first):
                self.dim_ops, self.wide_first = dim_ops, wide_first
                self.axis = 1 if wide_first else 0
                self.ff_ops, self.send, self.keep, self.chip, self.rows, self.full = {}, {}, {}, {}, {}, {}

            def link(self, color, second):
                return "dz" if (color == 0) == second else "dy"

            def product(self, color, send):
                ops = self.ff_ops[color]
                offset = color if ops[0].shape[1] > half_ff else 0
                part, own = grad_blocks([self.dim_ops[m] for m in (0, 1)], [at(ops[0]), ops[1]], ids[color, send], offset, self.wide_first, block)
                mark(own)
                got = lax.ppermute(part, "dx", SWAP)
                (self.send if send else self.keep)[color] = (own, got)

            def add_chip(self, color):
                own, got = self.send[color]
                chip = mark(at(own) + got)
                self.chip[color] = lax.ppermute(chip, self.link(color, False), SWAP)

            def add_rows(self, color):
                own, got = self.keep[color]
                total = mark(at(own) + got + self.chip[color])
                out, kept = jnp.split(total, 2, axis=self.axis)
                self.rows[color] = (kept, lax.ppermute(out, self.link(color, True), SWAP))

            def gather(self, color):
                kept, got = self.rows[color]
                shard = mark(at(kept) + got)
                self.full[color] = lax.all_gather(shard, ("dx", "dz", "dy"), axis=self.axis, tiled=True)

            def result(self):
                parts = [at(self.full[0]), self.full[1]]
                return mark(jnp.concatenate(parts, axis=1 - self.axis) / dev_count)

        def half(mat, color, axis):
            return lax.slice_in_dim(mat, color * half_ff, (color + 1) * half_ff, axis=axis)

        x_rows, g_rows = [x_one, x_two], [g_one, g_two]
        pre_one, act_one, act_two, dh_two, dx_rows = {}, {}, {}, {}, {}
        pre_three, act_three, dz_three, dz_one = ({0: {}, 1: {}} for _ in range(4))

        def forward_one(m):
            pre = mat_nn(x_rows[m], at(w_one)).astype(jnp.bfloat16)
            pre_one[m], act_one[m] = lax.optimization_barrier((pre, gelu_value(pre).astype(jnp.bfloat16)))
            mark(act_one[m])

        def forward_two(m):
            act_two[m] = mark((mat_nn(act_one[m], at(w_two)) + x_rows[m].astype(jnp.float32)).astype(jnp.bfloat16))

        def forward_three(color, m):
            pre = mat_nn(act_two[m], half(at(w_three), color, 1)).astype(jnp.bfloat16)
            pre_three[color][m], act_three[color][m] = lax.optimization_barrier((pre, gelu_value(pre).astype(jnp.bfloat16)))
            mark(act_three[color][m])

        def back_three(color, m):
            dz = mat_nt(g_rows[m], half(at(w_four), color, 0)) * gelu_slope(pre_three[color][m])
            dz_three[color][m] = mark(dz.astype(jnp.bfloat16))

        def back_two(m):
            weight = at(w_three)
            terms = mat_nt(dz_three[0][m], half(weight, 0, 1)) + mat_nt(dz_three[1][m], half(weight, 1, 1))
            dh_two[m] = mark((terms + g_rows[m].astype(jnp.float32)).astype(jnp.bfloat16))

        def back_one(color, m):
            dz = mat_nt(dh_two[m], half(at(w_two), color, 0)) * gelu_slope(half(pre_one[m], color, 1))
            dz_one[color][m] = mark(dz.astype(jnp.bfloat16))

        def back_x(m):
            weight = at(w_one)
            terms = mat_nt(dz_one[0][m], half(weight, 0, 1)) + mat_nt(dz_one[1][m], half(weight, 1, 1))
            dx_rows[m] = mark((terms + dh_two[m].astype(jnp.float32)).astype(jnp.bfloat16))

        four = Grad(g_rows, True)
        three = Grad(act_two, False)
        two = Grad(dh_two, True)
        one = Grad(x_rows, False)
        four.ff_ops, three.ff_ops, one.ff_ops = act_three, dz_three, dz_one
        two.ff_ops = {0: act_one, 1: act_one}
        grads = {4: four, 3: three, 2: two, 1: one}
        compute = {"F1": forward_one, "F2": forward_two, "F3": forward_three, "B3": back_three, "B2": back_two, "B1": back_one, "BX": back_x}
        results = {}
        for name, *args in STEPS:
            if name in compute:
                compute[name](*args)
            elif name in "SK":
                grads[args[0]].product(args[1], name == "S")
            elif name == "C":
                grads[args[0]].add_chip(args[1])
            elif name == "U":
                grads[args[0]].add_rows(args[1])
            elif name == "G":
                grads[args[0]].gather(args[1])
            else:
                results[args[0]] = grads[args[0]].result()
        return results[1], results[2], results[3], results[4], dx_rows[0], dx_rows[1]

    return jax.shard_map(
        per_device,
        mesh=mesh,
        in_specs=(row_spec, row_spec, row_spec, row_spec, rep_spec, rep_spec, rep_spec, rep_spec),
        out_specs=(rep_spec, rep_spec, rep_spec, rep_spec, row_spec, row_spec),
        check_vma=False,
    )
```

```python
import jax
import jax.numpy as jnp
from jax import lax
from jax.experimental import pallas as pl
from jax.experimental.pallas import tpu as pltpu
from jax.sharding import PartitionSpec as P

GELU_C = 0.7978845608028654
GELU_A = 0.044715
SWAP = [(0, 1), (1, 0)]
FF_TILE = 512


STEPS = (
    ("F1", 0), ("F1", 1), ("F2", 0), ("F2", 1),
    ("F3", 0, 0), ("F3", 0, 1), ("S", 4, 0), ("F3", 1, 0), ("C", 4, 0), ("F3", 1, 1), ("S", 4, 1), ("K", 4, 0), ("C", 4, 1), ("K", 4, 1),
    ("U", 4, 0), ("B3", 0, 0), ("B3", 0, 1), ("U", 4, 1), ("S", 3, 0), ("B3", 1, 0), ("C", 3, 0), ("G", 4, 0), ("B3", 1, 1), ("G", 4, 1), ("S", 3, 1),
    ("K", 3, 0), ("C", 3, 1), ("K", 3, 1), ("B2", 0), ("B2", 1), ("U", 3, 0), ("S", 2, 0), ("S", 2, 1), ("C", 2, 0), ("B1", 0, 0), ("G", 3, 0),
    ("C", 2, 1), ("U", 3, 1), ("B1", 0, 1), ("S", 1, 0), ("K", 2, 0), ("C", 1, 0), ("G", 3, 1), ("B1", 1, 0), ("U", 2, 0), ("B1", 1, 1), ("S", 1, 1), ("K", 2, 1), ("C", 1, 1),
    ("U", 2, 1), ("K", 1, 0), ("G", 2, 0), ("K", 1, 1), ("BX", 0), ("G", 2, 1), ("U", 1, 0), ("BX", 1), ("U", 1, 1), ("R", 4),
    ("G", 1, 0), ("R", 3), ("G", 1, 1), ("R", 2), ("Q", 1), ("R", 1),
)


def gelu_value(pre_act):
    pre_f = pre_act.astype(jnp.float32)
    return 0.5 * pre_f * (1.0 + jnp.tanh(GELU_C * (pre_f + GELU_A * pre_f * pre_f * pre_f)))


def gelu_slope(pre_act):
    pre_f = pre_act.astype(jnp.float32)
    square = pre_f * pre_f
    tanh_val = jnp.tanh(pre_f * (GELU_C + (GELU_C * GELU_A) * square))
    return (0.5 + 0.5 * tanh_val) * (1.0 + (pre_f * (1.0 - tanh_val)) * (GELU_C + (3.0 * GELU_C * GELU_A) * square))


def mat_nn(left_op, right_op):
    return jnp.dot(left_op, right_op, preferred_element_type=jnp.float32)


def mat_nt(left_op, right_op):
    return lax.dot_general(left_op, right_op, (((1,), (1,)), ((), ())), preferred_element_type=jnp.float32)


def mat_tn(left_op, right_op):
    return lax.dot_general(left_op, right_op, (((0,), (0,)), ((), ())), preferred_element_type=jnp.float32)


def grad_blocks(dim_ops, ff_ops, blocks, offset, wide_first, block):
    count = len(dim_ops)
    rows = dim_ops[0].shape[0]
    half = 10 * block
    tiles = half // FF_TILE

    def body(blocks_ref, *refs):
        dim_refs, ff_refs, out_refs = refs[: 4 * count], refs[4 * count : 5 * count], refs[5 * count :]
        for i in range(4):
            value = None
            for m in range(count):
                dim_val, ff_val = dim_refs[4 * m + i][...], ff_refs[m][...]
                term = mat_tn(ff_val, dim_val) if wide_first else mat_tn(dim_val, ff_val)
                value = term if value is None else value + term
            lo = (i % 2) * block
            if wide_first:
                out_refs[i // 2][:, lo : lo + block] = value
            else:
                out_refs[i // 2][lo : lo + block, :] = value

    def dim_spec(i):
        return pl.BlockSpec((rows, block), lambda j, b: (0, b[i]))

    if wide_first:
        out_shape = jax.ShapeDtypeStruct((half, 2 * block), jnp.float32)
        out_spec = pl.BlockSpec((FF_TILE, 2 * block), lambda j, b: (j, 0))
    else:
        out_shape = jax.ShapeDtypeStruct((2 * block, half), jnp.float32)
        out_spec = pl.BlockSpec((2 * block, FF_TILE), lambda j, b: (0, j))
    return pl.pallas_call(
        body,
        grid_spec=pltpu.PrefetchScalarGridSpec(
            num_scalar_prefetch=1,
            grid=(tiles,),
            in_specs=[dim_spec(i) for _ in range(count) for i in range(4)]
            + [pl.BlockSpec((rows, FF_TILE), lambda j, b: (0, offset * tiles + j)) for _ in range(count)],
            out_specs=[out_spec, out_spec],
        ),
        out_shape=[out_shape, out_shape],
        compiler_params=pltpu.CompilerParams(vmem_limit_bytes=62 * 1024 * 1024, dimension_semantics=("arbitrary",)),
        cost_estimate=pl.CostEstimate(flops=8 * count * rows * block * half, bytes_accessed=2 * count * rows * (half + 4 * block) + 16 * block * half, transcendentals=0),
    )(blocks, *[op for op in dim_ops for _ in range(4)], *ff_ops)


def solution(mesh):
    dev_count = mesh.shape["dz"] * mesh.shape["dy"] * mesh.shape["dx"]
    row_spec = P(("dz", "dy", "dx"), None)
    rep_spec = P(None, None)

    def per_device(x_one, g_one, x_two, g_two, w_one, w_two, w_three, w_four):
        dim, ff = w_one.shape
        block = dim // dev_count
        half_ff = ff // 2
        idx_z, idx_y, idx_c = lax.axis_index("dz"), lax.axis_index("dy"), lax.axis_index("dx")
        anchor = [x_one]

        def at(*vals):
            out = lax.optimization_barrier((*vals, anchor[0]))[:-1]
            return out if len(out) > 1 else out[0]

        def mark(val):
            anchor[0] = val
            return val

        def block_ids(color, send):
            ids = []
            for core in (1 - idx_c, idx_c):
                if color == 0:
                    col = 1 - idx_y if send else idx_y
                    ids += [4 * core + 2 * (1 - idx_z) + col, 4 * core + 2 * idx_z + col]
                else:
                    row = 1 - idx_z if send else idx_z
                    ids += [4 * core + 2 * row + 1 - idx_y, 4 * core + 2 * row + idx_y]
            return jnp.stack(ids).astype(jnp.int32)

        ids = {(color, send): block_ids(color, send) for color in (0, 1) for send in (False, True)}

        class Grad:
            def __init__(self, dim_ops, wide_first):
                self.dim_ops, self.wide_first = dim_ops, wide_first
                self.axis = 1 if wide_first else 0
                self.base = None
                self.ff_ops, self.send, self.keep, self.chip, self.rows, self.full = {}, {}, {}, {}, {}, {}

            def link(self, color, second):
                return "dz" if (color == 0) == second else "dy"

            def product(self, color, send):
                ops = self.ff_ops[color]
                offset = color if ops[0].shape[1] > half_ff else 0
                part, own = grad_blocks([self.dim_ops[m] for m in (0, 1)], [at(ops[0]), ops[1]], ids[color, send], offset, self.wide_first, block)
                mark(own)
                got = lax.ppermute(part, "dx", SWAP)
                (self.send if send else self.keep)[color] = (own, got)

            def add_chip(self, color):
                own, got = self.send[color]
                chip = mark(at(own) + got)
                self.chip[color] = lax.ppermute(chip, self.link(color, False), SWAP)

            def add_rows(self, color):
                own, got = self.keep[color]
                total = mark(at(own) + got + self.chip[color])
                out, kept = jnp.split(total, 2, axis=self.axis)
                self.rows[color] = (kept, lax.ppermute(out, self.link(color, True), SWAP))

            def gather(self, color):
                kept, got = self.rows[color]
                shard = mark(at(kept) + got)
                self.full[color] = lax.all_gather(shard, ("dx", "dz", "dy"), axis=self.axis, tiled=True)

            def begin(self):
                pads = [(0, 0), (0, 0)]
                pads[1 - self.axis] = (0, half_ff)
                self.base = mark(jnp.pad(at(self.full[0]) / dev_count, pads))

            def result(self):
                if self.base is not None:
                    return mark(lax.dynamic_update_slice_in_dim(at(self.base), self.full[1] / dev_count, half_ff, axis=1 - self.axis))
                parts = [at(self.full[0]), self.full[1]]
                return mark(jnp.concatenate(parts, axis=1 - self.axis) / dev_count)

        def half(mat, color, axis):
            return lax.slice_in_dim(mat, color * half_ff, (color + 1) * half_ff, axis=axis)

        x_rows, g_rows = [x_one, x_two], [g_one, g_two]
        pre_one, act_one, act_two, dh_two, dx_rows = {}, {}, {}, {}, {}
        pre_three, act_three, dz_three, dz_one = ({0: {}, 1: {}} for _ in range(4))

        def forward_one(m):
            pre = mat_nn(x_rows[m], at(w_one)).astype(jnp.bfloat16)
            pre_one[m], act_one[m] = lax.optimization_barrier((pre, gelu_value(pre).astype(jnp.bfloat16)))
            mark(act_one[m])

        def forward_two(m):
            act_two[m] = mark((mat_nn(act_one[m], at(w_two)) + x_rows[m].astype(jnp.float32)).astype(jnp.bfloat16))

        def forward_three(color, m):
            pre = mat_nn(act_two[m], half(at(w_three), color, 1)).astype(jnp.bfloat16)
            pre_three[color][m], act_three[color][m] = lax.optimization_barrier((pre, gelu_value(pre).astype(jnp.bfloat16)))
            mark(act_three[color][m])

        def back_three(color, m):
            dz = mat_nt(g_rows[m], half(at(w_four), color, 0)) * gelu_slope(pre_three[color][m])
            dz_three[color][m] = mark(dz.astype(jnp.bfloat16))

        def back_two(m):
            weight = at(w_three)
            terms = mat_nt(dz_three[0][m], half(weight, 0, 1)) + mat_nt(dz_three[1][m], half(weight, 1, 1))
            dh_two[m] = mark((terms + g_rows[m].astype(jnp.float32)).astype(jnp.bfloat16))

        def back_one(color, m):
            dz = mat_nt(dh_two[m], half(at(w_two), color, 0)) * gelu_slope(half(pre_one[m], color, 1))
            dz_one[color][m] = mark(dz.astype(jnp.bfloat16))

        def back_x(m):
            weight = at(w_one)
            terms = mat_nt(dz_one[0][m], half(weight, 0, 1)) + mat_nt(dz_one[1][m], half(weight, 1, 1))
            dx_rows[m] = mark((terms + dh_two[m].astype(jnp.float32)).astype(jnp.bfloat16))

        four = Grad(g_rows, True)
        three = Grad(act_two, False)
        two = Grad(dh_two, True)
        one = Grad(x_rows, False)
        four.ff_ops, three.ff_ops, one.ff_ops = act_three, dz_three, dz_one
        two.ff_ops = {0: act_one, 1: act_one}
        grads = {4: four, 3: three, 2: two, 1: one}
        compute = {"F1": forward_one, "F2": forward_two, "F3": forward_three, "B3": back_three, "B2": back_two, "B1": back_one, "BX": back_x}
        results = {}
        for name, *args in STEPS:
            if name in compute:
                compute[name](*args)
            elif name in "SK":
                grads[args[0]].product(args[1], name == "S")
            elif name == "C":
                grads[args[0]].add_chip(args[1])
            elif name == "U":
                grads[args[0]].add_rows(args[1])
            elif name == "G":
                grads[args[0]].gather(args[1])
            elif name == "Q":
                grads[args[0]].begin()
            else:
                results[args[0]] = grads[args[0]].result()
        return results[1], results[2], results[3], results[4], dx_rows[0], dx_rows[1]

    return jax.shard_map(
        per_device,
        mesh=mesh,
        in_specs=(row_spec, row_spec, row_spec, row_spec, rep_spec, rep_spec, rep_spec, rep_spec),
        out_specs=(rep_spec, rep_spec, rep_spec, rep_spec, row_spec, row_spec),
        check_vma=False,
    )
```
